32 devices in a mesh: seq: 2 (over y), section: 4 (over x, core), tp: 4 (over z).
Axes of the slice: x: 2, y: 2, z: 4, core: 2. Of those that a mesh axis runs over, the one named last changes fastest.
Arguments:
- token_ids: int32 [128], P('seq'), may hold values from 0 to 65535
- embed_columns: bfloat16 [4096, 65536], P(('tp', 'seq')), may hold values from -6 to 6
- norm_gain: bfloat16 [4, 4096], P('section'), may hold values from 0.099609375 to 1.8984375
- qkv_weight: bfloat16 [4, 4096, 4096], P('section', 'seq', 'tp'), may hold values from -1 to 1
- out_weight: bfloat16 [4, 4096, 2048], P('section', 'seq', 'tp'), may hold values from -0.125 to 0.125
Outputs:
- layer_states: bfloat16 [4, 128, 4096], P('section', 'seq', 'tp')
The draws below stay inside these ranges and needn't reach their ends.
All inputs are finite; a program needn't handle non-finite values.
Results may differ from the reference program's by a relative error of at most 0.02.
Values may be sent and summed in bfloat16 or wider, within the bound.
A program may use at most 192 MiB of HBM per device.

```python
import math
import jax
import jax.numpy as jnp
import numpy as np
from jax import lax

D = 4096
QUERY_HEADS = 16
KEY_VALUE_HEADS = 8
HEAD_WIDTH = 128
VOCAB = 65536
BLOCK = 64
LAYERS = 4
CONTEXT_TOKENS = 128
N_SEQ = 2
N_TP = 4


def draw_qkv_weight(key, part):
    group_factor = N_TP
    query_heads = QUERY_HEADS // group_factor
    key_value_heads = KEY_VALUE_HEADS // group_factor
    drawn = jax.random.normal(key, (LAYERS, D, group_factor, query_heads + 2 * key_value_heads, HEAD_WIDTH), jnp.float32) * D ** (-0.5)
    drawn = jnp.clip(drawn, -1.0, 1.0)
    return drawn.reshape(LAYERS, D, group_factor * (query_heads + 2 * key_value_heads) * HEAD_WIDTH).astype(jnp.bfloat16)


def plant(values, key, least, top_value):
    index_at = [jax.random.randint(jax.random.fold_in(key, axis), (), 0, length) for axis, length in enumerate(values.shape)]
    widest = values.shape.index(max(values.shape))
    next_to = index_at[:widest] + [(index_at[widest] + 1) % values.shape[widest]] + index_at[widest + 1:]
    return values.at[tuple(index_at)].set(least).at[tuple(next_to)].set(top_value)


def level_of(stream_key, dims, split, low, top_value):
    loudness, own = 1.0, jax.random.fold_in(stream_key, 6)
    for dim, blocks in split:
        draws = jnp.exp(jax.random.uniform(jax.random.fold_in(own, dim), (blocks,), jnp.float32, low / len(split), top_value / len(split)))
        loudness = loudness * jnp.repeat(draws, dims[dim] // blocks).reshape([-1 if axis == dim else 1 for axis in range(len(dims))])
    return loudness


def cumulative_ranks(count, lean):
    portions = [(1 << 20) // math.isqrt(standing ** lean) + 1 for standing in range(1, count + 1)]
    scale = 1 + sum(portions) // (1 << 30)
    return np.cumsum(np.array([max(1, weight // scale) for weight in portions]))


def skewed_ids(own_key, extent, amount, lean):
    grid = cumulative_ranks(amount, lean)
    pick = jax.random.randint(jax.random.fold_in(own_key, 1), extent, 0, int(grid[amount - 1]))
    grade = jnp.searchsorted(jnp.asarray(grid, jnp.int32), pick, side="right")
    return jax.random.permutation(jax.random.fold_in(own_key, 2), amount)[grade].astype(jnp.int32)


def bell_draw(stream_key, shape, scale, limit, pieces=(), kind=jnp.bfloat16):
    array = scale * jax.random.normal(stream_key, shape, jnp.float32)
    if pieces:
        array = array * level_of(stream_key, shape, pieces, -0.22, 0.18)
    return jnp.clip(array, -limit, limit).astype(kind)


def setup_inputs(seed: int = 0) -> dict:
    splits = jax.random.split(jax.random.key(seed), 6)
    return {
        "token_ids": plant(skewed_ids(splits[0], (CONTEXT_TOKENS,), VOCAB, 2), jax.random.fold_in(splits[0], 3), 0, VOCAB - 1).astype(jnp.int32),
        "embed_columns": bell_draw(splits[1], (D, VOCAB), 1.0, 6.0, ((0, 8),)),
        "norm_gain": jnp.clip(1.0 + 0.18 * jax.random.normal(splits[2], (LAYERS, D), jnp.float32), 0.099609375, 1.8984375).astype(jnp.bfloat16),
        "qkv_weight": draw_qkv_weight(jax.random.fold_in(splits[5], 71), 0),
        "out_weight": bell_draw(splits[4], (LAYERS, D, QUERY_HEADS * HEAD_WIDTH), (QUERY_HEADS * HEAD_WIDTH) ** -0.5, 0.125, ((0, 4), (1, 2), (2, 4))),
    }


EPS = 1e-05
ROPE_BASE = 500000.0
MASKED = -1e+30

def rope_tables(positions, head_size):
    half_width = head_size // 2
    inverse_freq = ROPE_BASE ** (-jnp.arange(half_width).astype(jnp.float32) * (2.0 / head_size))
    angles = positions.astype(jnp.float32)[:, None] * inverse_freq[None, :]
    return (jnp.cos(angles), jnp.sin(angles))

def rotate_half(heads, cosine_table, sine_values):
    half_width = heads.shape[-1] // 2
    first_half = heads[..., :half_width]
    second = heads[..., half_width:]
    cosine_table = cosine_table[:, None, :]
    sine_values = sine_values[:, None, :]
    return jnp.concatenate([first_half * cosine_table - second * sine_values, second * cosine_table + first_half * sine_values], axis=-1)

def norm_rows(row_block, gain_row):
    values = row_block.astype(jnp.float32)
    inverse_rms = lax.rsqrt(lax.optimization_barrier(jnp.mean(values * values, axis=-1, keepdims=True)) + EPS)
    return (values * inverse_rms * gain_row.astype(jnp.float32)[None, :]).astype(jnp.bfloat16)

def reference(token_ids, embed_columns, norm_gain, qkv_weight, out_weight):
    group_factor = N_SEQ
    block_row_slice = BLOCK
    query_heads = QUERY_HEADS // N_TP
    key_value_heads = KEY_VALUE_HEADS // N_TP
    repeat_heads = QUERY_HEADS // KEY_VALUE_HEADS
    hidden = jnp.take(embed_columns, token_ids, axis=1).T
    positions = jnp.arange(CONTEXT_TOKENS).astype(jnp.int32)
    cosine_table, sine_values = rope_tables(positions, HEAD_WIDTH)
    row_ids = jnp.arange(block_row_slice)[None, :, None]
    column = jnp.arange(2 * block_row_slice)[None, None, :]
    group_ids = jnp.arange(group_factor)[:, None, None]
    allowed = jnp.where(column < block_row_slice, group_ids > 0, column - block_row_slice <= row_ids)
    states = []
    for layer_index in range(LAYERS):
        normed = norm_rows(hidden, norm_gain[layer_index])
        projected_rows = jnp.dot(normed, qkv_weight[layer_index], preferred_element_type=jnp.float32)
        projected_rows = projected_rows.reshape(CONTEXT_TOKENS, N_TP, query_heads + 2 * key_value_heads, HEAD_WIDTH)
        query_rows = rotate_half(projected_rows[:, :, :query_heads].reshape(CONTEXT_TOKENS, QUERY_HEADS, HEAD_WIDTH), cosine_table, sine_values).astype(jnp.bfloat16)
        key_head_rows = rotate_half(projected_rows[:, :, query_heads:query_heads + key_value_heads].reshape(CONTEXT_TOKENS, KEY_VALUE_HEADS, HEAD_WIDTH), cosine_table, sine_values).astype(jnp.bfloat16)
        value_head_rows = projected_rows[:, :, query_heads + key_value_heads:].reshape(CONTEXT_TOKENS, KEY_VALUE_HEADS, HEAD_WIDTH).astype(jnp.bfloat16)
        key_head_rows = key_head_rows.reshape(group_factor, block_row_slice, KEY_VALUE_HEADS, HEAD_WIDTH)
        value_head_rows = value_head_rows.reshape(group_factor, block_row_slice, KEY_VALUE_HEADS, HEAD_WIDTH)
        both_keys = jnp.concatenate([jnp.broadcast_to(key_head_rows[:1], key_head_rows.shape), key_head_rows], axis=1)
        both_values = jnp.concatenate([jnp.broadcast_to(value_head_rows[:1], value_head_rows.shape), value_head_rows], axis=1)
        query_groups = query_rows.reshape(group_factor, block_row_slice, KEY_VALUE_HEADS, repeat_heads, HEAD_WIDTH).astype(jnp.float32)
        scores = jnp.einsum('grkph,gckh->gkprc', query_groups, both_keys.astype(jnp.float32)) * HEAD_WIDTH ** (-0.5)
        scores = jnp.where(allowed[:, None, None], scores, MASKED)
        weights = jax.nn.softmax(scores, axis=-1).astype(jnp.bfloat16)
        attended = jnp.einsum('gkprc,gckh->grkph', weights.astype(jnp.float32), both_values.astype(jnp.float32)).astype(jnp.bfloat16)
        attended = attended.reshape(CONTEXT_TOKENS, N_TP, query_heads * HEAD_WIDTH)
        out_heads = out_weight[layer_index].reshape(D, N_TP, query_heads * HEAD_WIDTH)
        partial_value = jnp.einsum('rtc,dtc->trd', attended.astype(jnp.float32), out_heads.astype(jnp.float32)).astype(jnp.bfloat16)
        partial_value = lax.optimization_barrier(partial_value)
        summed = lax.optimization_barrier(jnp.sum(partial_value.astype(jnp.float32), axis=0))
        hidden = (hidden.astype(jnp.float32) + summed).astype(jnp.bfloat16)
        states.append(hidden)
    return jnp.stack(states)
```

```python
import functools

import jax
import jax.numpy as jnp
from jax import lax
from jax.experimental import pallas as pl
from jax.experimental.pallas import tpu as pltpu
from jax.sharding import PartitionSpec as P

QUERY_HEADS = 16
KEY_VALUE_HEADS = 8
HEAD_WIDTH = 128


EPS = 1e-05
ROPE_BASE = 500000.0
MASKED = -1e30


def passed_along(value, axis, steps):
    count = lax.axis_size(axis)
    leading, last = (max(0, -steps), min(count, count - steps))
    return lax.ppermute(value, axis, [(source, source + steps) for source in range(leading, last)])


def from_root(value, axis, root):
    mine = lax.axis_index(axis) == root
    return lax.psum(jnp.where(mine, value, jnp.zeros_like(value)), axis)


def rope_tables(positions, head_size):
    half_width = head_size // 2
    inverse_freq = ROPE_BASE ** (-jnp.arange(half_width).astype(jnp.float32) * (2.0 / head_size))
    angles = positions.astype(jnp.float32)[:, None] * inverse_freq[None, :]
    return (jnp.cos(angles), jnp.sin(angles))


def rotate_half(heads, cosine_table, sine_values):
    half_width = heads.shape[-1] // 2
    first_half = heads[..., :half_width]
    second = heads[..., half_width:]
    cosine_table = cosine_table[:, None, :]
    sine_values = sine_values[:, None, :]
    return jnp.concatenate(
        [
            first_half * cosine_table - second * sine_values,
            second * cosine_table + first_half * sine_values,
        ],
        axis=-1,
    )


def norm_rows(row_block, gain_row):
    values = row_block.astype(jnp.float32)
    inverse_rms = lax.rsqrt(jnp.mean(values * values, axis=-1, keepdims=True) + EPS)
    return (values * inverse_rms * gain_row[None, :]).astype(jnp.bfloat16)


def widen(current):
    return lax.all_gather(current, "tp", axis=1, tiled=True)


def project(full_rows, gain_row, qkv_full, positions, query_heads, key_value_heads):
    row_count = full_rows.shape[0]
    normed = norm_rows(full_rows, gain_row)
    projected_rows = jnp.dot(normed, qkv_full, preferred_element_type=jnp.float32)
    projected_rows = projected_rows.reshape(
        row_count, query_heads + 2 * key_value_heads, HEAD_WIDTH
    )
    cosine_table, sine_values = rope_tables(positions, HEAD_WIDTH)
    query_rows = rotate_half(projected_rows[:, :query_heads], cosine_table, sine_values).astype(
        jnp.bfloat16
    )
    key_head_rows = rotate_half(
        projected_rows[:, query_heads : query_heads + key_value_heads], cosine_table, sine_values
    ).astype(jnp.bfloat16)
    value_head_rows = projected_rows[:, query_heads + key_value_heads :].astype(jnp.bfloat16)
    return (query_rows, key_head_rows, value_head_rows)


def attend(query_rows, key_head_rows, value_head_rows, allowed):
    row_count, query_heads, head_size = query_rows.shape
    key_value_heads = key_head_rows.shape[1]
    query_groups = query_rows.reshape(
        row_count, key_value_heads, query_heads // key_value_heads, head_size
    )
    scores = jnp.einsum(
        "rkph,ckh->kprc", query_groups, key_head_rows, preferred_element_type=jnp.float32
    ) * head_size ** (-0.5)
    scores = jnp.where(allowed[None, None], scores, MASKED)
    weights = jax.nn.softmax(scores, axis=-1).astype(jnp.bfloat16)
    attended = jnp.einsum(
        "kprc,ckh->rkph", weights, value_head_rows, preferred_element_type=jnp.float32
    )
    return attended.reshape(row_count, query_heads * head_size).astype(jnp.bfloat16)


def combine(current, attended, out_full):
    partial_value = lax.dot_general(
        attended, out_full, (((1,), (1,)), ((), ())), preferred_element_type=jnp.float32
    )
    summed = lax.psum_scatter(
        partial_value.astype(jnp.bfloat16), "tp", scatter_dimension=1, tiled=True
    ).astype(jnp.float32)
    return (current.astype(jnp.float32) + summed).astype(jnp.bfloat16)


def advance(new_rows):
    return passed_along(new_rows, "section", 1)


def body(token_ids, embed_columns, norm_gain, qkv_weight, out_weight):
    seq_count = lax.axis_size("seq")
    section_count = lax.axis_size("section")
    tensor_parallel_count = lax.axis_size("tp")
    group_index = lax.axis_index("seq")
    section_index = lax.axis_index("section")
    block_row_slice = token_ids.shape[0]
    feature_slice = embed_columns.shape[0]
    feature_cols = feature_slice * seq_count
    query_heads = QUERY_HEADS // tensor_parallel_count
    key_value_heads = KEY_VALUE_HEADS // tensor_parallel_count
    every_id = lax.all_gather(token_ids, "seq", axis=0, tiled=True)
    looked = jnp.take(embed_columns, every_id, axis=1)
    arrived = lax.all_to_all(looked, "seq", split_axis=1, concat_axis=0, tiled=True)
    residual = arrived.T
    qkv_full, out_full = (
        lax.all_gather(qkv_weight, "seq", axis=1, tiled=True),
        lax.all_gather(out_weight, "seq", axis=1, tiled=True),
    )
    qkv_full = qkv_full[0]
    out_full = out_full[0]
    gain_row = norm_gain[0].astype(jnp.float32)
    outputs = jnp.zeros((block_row_slice, feature_cols), jnp.bfloat16)
    row_ids = jnp.arange(block_row_slice)[:, None]
    column = jnp.arange(2 * block_row_slice)[None, :]
    positions = group_index * block_row_slice + jnp.arange(block_row_slice)
    allowed = jnp.where(
        column < block_row_slice, group_index > 0, column - block_row_slice <= row_ids
    )
    current = residual
    for step_number in range(section_count):
        query_rows, key_head_rows, value_head_rows = project(
            widen(current), gain_row, qkv_full, positions, query_heads, key_value_heads
        )
        anchor_heads, anchor_values = (
            from_root(key_head_rows, "seq", 0),
            from_root(value_head_rows, "seq", 0),
        )
        both_keys = jnp.concatenate([anchor_heads, key_head_rows], axis=0)
        both_values = jnp.concatenate([anchor_values, value_head_rows], axis=0)
        attended = attend(query_rows, both_keys, both_values, allowed)
        new_rows = combine(current, attended, out_full)
        outputs = jnp.where(section_index == step_number, new_rows, outputs)
        if step_number + 1 < section_count:
            current = advance(new_rows)
    return outputs[None]


LANES = 128
TOKEN_GROUP = 8
MESH = pl.DeviceIdType.MESH


def lookup_kernel(ids_ref, table_ref, out_ref, tiles, sems):
    count = out_ref.shape[0]
    width = table_ref.shape[0]
    first = lax.axis_index("section") * count

    def fetch(i):
        start = pl.multiple_of((ids_ref[first + i] // LANES) * LANES, LANES)
        return pltpu.make_async_copy(
            table_ref.at[:, pl.ds(start, LANES)], tiles.at[:, pl.ds(i * LANES, LANES)], sems.at[i]
        )

    for i in range(count):
        fetch(i).start()
    rows = lax.broadcasted_iota(jnp.int32, (LANES, LANES), 0)
    columns = lax.broadcasted_iota(jnp.int32, (LANES, LANES), 1)
    total = jnp.zeros((width, LANES), jnp.float32)
    group = min(TOKEN_GROUP, count)
    for base in range(0, count, group):
        picks = []
        for i in range(base, base + group):
            chosen = jnp.logical_and(rows == ids_ref[first + i] % LANES, columns == i)
            picks.append(jnp.where(chosen, 1.0, 0.0).astype(jnp.bfloat16))
        pick = jnp.concatenate(picks, axis=0)
        for i in range(base, base + group):
            fetch(i).wait()
        total += jnp.dot(
            tiles[:, base * LANES : (base + group) * LANES], pick, preferred_element_type=jnp.float32
        )
    out_ref[...] = total.T[:count].astype(jnp.bfloat16)


def chain_kernel(
    n_seq,
    n_sec,
    n_tp,
    piece_ref,
    gain_ref,
    cos_ref,
    sin_ref,
    qkv_ref,
    outw_ref,
    out_ref,
    wq,
    wo,
    hidden,
    acc,
    part_send,
    part_recv,
    sq_send,
    sq_recv,
    heads,
    rs_send,
    rs_recv,
    fresh,
    w_sem,
    h_ssem,
    h_rsem,
    p_ssem,
    p_rsem,
    q_ssem,
    q_rsem,
    r_ssem,
    r_rsem,
    o_ssem,
    o_rsem,
):
    seq, sec, tp = (lax.axis_index(a) for a in ("seq", "section", "tp"))
    other = 1 - seq
    tokens, chunk = fresh.shape
    piece = tokens // n_sec
    block = out_ref.shape[1]
    groups, _, group_width = part_send.shape
    query_heads = QUERY_HEADS // n_tp
    kv_heads = KEY_VALUE_HEADS // n_tp

    load_q = [
        pltpu.make_async_copy(
            qkv_ref.at[0, pl.ds(((tp + d) % n_tp) * chunk, chunk), :],
            wq.at[pl.ds(((tp + d) % n_tp) * chunk, chunk), :],
            w_sem.at[d],
        )
        for d in range(n_tp)
    ]
    load_o = pltpu.make_async_copy(outw_ref.at[0], wo, w_sem.at[n_tp])
    for c in load_q:
        c.start()
    load_o.start()

    shard = tp * n_seq + seq
    half, slot = shard // n_tp, shard % n_tp

    def seed_copy(j):
        return pltpu.make_async_remote_copy(
            src_ref=piece_ref,
            dst_ref=hidden.at[slot, pl.ds(sec * piece, piece), :],
            send_sem=h_ssem.at[0, j],
            recv_sem=h_rsem.at[slot, sec],
            device_id={"seq": half, "section": 0, "tp": j},
            device_id_type=MESH,
        )

    def seed_is_mine(j):
        return jnp.logical_and(sec == 0, jnp.logical_and(half == seq, tp == j))

    seed_local = pltpu.make_async_copy(
        piece_ref, hidden.at[slot, pl.ds(sec * piece, piece), :], h_rsem.at[slot, sec]
    )
    for j in range(n_tp):
        mine = seed_is_mine(j)

        @pl.when(mine)
        def _():
            seed_local.start()

        @pl.when(jnp.logical_not(mine))
        def _():
            seed_copy(j).start()

    squares = jnp.zeros((tokens, LANES), jnp.float32)
    for d in range(n_tp):
        c = (tp + d) % n_tp
        for k in range(n_sec):
            pltpu.make_async_copy(
                hidden.at[c, pl.ds(k * piece, piece), :],
                hidden.at[c, pl.ds(k * piece, piece), :],
                h_rsem.at[c, k],
            ).wait()
        load_q[d].wait()
        rows = hidden[c].astype(jnp.float32)
        sq = rows * rows
        for k in range(chunk // LANES):
            squares += sq[:, k * LANES : (k + 1) * LANES]
        scaled = (rows * gain_ref[pl.ds(c, 1), :]).astype(jnp.bfloat16)
        if d == n_tp - 1:
            sq_send[...] = squares
            sq_copy = pltpu.make_async_remote_copy(
                src_ref=sq_send,
                dst_ref=sq_recv,
                send_sem=q_ssem,
                recv_sem=q_rsem,
                device_id={"seq": other},
                device_id_type=MESH,
            )
            sq_copy.start()
        part_copies = []
        for g in range(groups):
            cols = slice(g * group_width, (g + 1) * group_width)
            product = jnp.dot(
                scaled,
                wq[pl.ds(pl.multiple_of(c * chunk, chunk), chunk), cols],
                preferred_element_type=jnp.float32,
            )
            if d > 0:
                product += acc[:, cols]
            acc[:, cols] = product
            if d == n_tp - 1:
                part_send[g] = product.astype(jnp.bfloat16)
                copy = pltpu.make_async_remote_copy(
                    src_ref=part_send.at[g],
                    dst_ref=part_recv.at[g],
                    send_sem=p_ssem.at[g],
                    recv_sem=p_rsem.at[g],
                    device_id={"seq": other},
                    device_id_type=MESH,
                )
                copy.start()
                part_copies.append(copy)

    sq_copy.wait_recv()
    features = n_seq * n_tp * chunk
    mean = jnp.sum(squares + sq_recv[...], axis=-1, keepdims=True) * (1.0 / features)
    inverse_rms = lax.rsqrt(mean + EPS)
    cosine, sine = cos_ref[...], sin_ref[...]
    ready = []
    for g in range(groups):
        part_copies[g].wait_recv()
        cols = slice(g * group_width, (g + 1) * group_width)
        whole = (acc[:, cols] + part_recv[g].astype(jnp.float32)) * inverse_rms
        for k in range(group_width // HEAD_WIDTH):
            head = whole[:, k * HEAD_WIDTH : (k + 1) * HEAD_WIDTH]
            if len(ready) < query_heads + kv_heads:
                head = head * cosine + pltpu.roll(head, HEAD_WIDTH // 2, 1) * sine
            ready.append(head.astype(jnp.bfloat16))

    repeat = query_heads // kv_heads
    row_at = lax.broadcasted_iota(jnp.int32, (tokens, tokens), 0)
    key_at = lax.broadcasted_iota(jnp.int32, (tokens, tokens), 1)
    visible = key_at <= row_at
    for h in range(query_heads):
        keys = ready[query_heads + h // repeat]
        values = ready[query_heads + kv_heads + h // repeat]
        scores = lax.dot_general(
            ready[h], keys, (((1,), (1,)), ((), ())), preferred_element_type=jnp.float32
        ) * HEAD_WIDTH ** (-0.5)
        scores = jnp.where(visible, scores, MASKED)
        shifted = jnp.exp(scores - jnp.max(scores, axis=-1, keepdims=True))
        weights = (shifted / jnp.sum(shifted, axis=-1, keepdims=True)).astype(jnp.bfloat16)
        heads[:, h * HEAD_WIDTH : (h + 1) * HEAD_WIDTH] = jnp.dot(
            weights, values, preferred_element_type=jnp.float32
        ).astype(jnp.bfloat16)

    load_o.wait()
    attended = heads[...]

    def rs_copy(d):
        return pltpu.make_async_remote_copy(
            src_ref=rs_send.at[d],
            dst_ref=rs_recv.at[d],
            send_sem=r_ssem.at[d],
            recv_sem=r_rsem.at[d],
            device_id={"tp": (tp + d) % n_tp},
            device_id_type=MESH,
        )

    own = None
    for d in [*range(1, n_tp), 0]:
        c = (tp + d) % n_tp
        partial = lax.dot_general(
            attended,
            wo[pl.ds(pl.multiple_of(c * chunk, chunk), chunk), :],
            (((1,), (1,)), ((), ())),
            preferred_element_type=jnp.float32,
        ).astype(jnp.bfloat16)
        if d:
            rs_send[d] = partial
            rs_copy(d).start()
        else:
            own = partial.astype(jnp.float32)
    summed = own
    for d in range(1, n_tp):
        rs_copy(d).wait_recv()
        summed += rs_recv[d].astype(jnp.float32)
    fresh[...] = (hidden[tp].astype(jnp.float32) + summed).astype(jnp.bfloat16)

    def next_copy(j, k):
        return pltpu.make_async_remote_copy(
            src_ref=fresh.at[pl.ds(k * piece, piece), :],
            dst_ref=hidden.at[tp, pl.ds(k * piece, piece), :],
            send_sem=h_ssem.at[k + 1, j],
            recv_sem=h_rsem.at[tp, k],
            device_id={"section": sec + 1, "tp": j},
            device_id_type=MESH,
        )

    @pl.when(sec < n_sec - 1)
    def _():
        for j in range(n_tp):
            for k in range(n_sec):
                next_copy(j, k).start()

    place = seq * n_tp + tp
    holder, part_of = place // n_seq, place % n_seq

    def out_copy(b):
        return pltpu.make_async_remote_copy(
            src_ref=fresh.at[pl.ds(b * block, block), :],
            dst_ref=out_ref.at[0, :, pl.ds(pl.multiple_of(part_of * chunk, chunk), chunk)],
            send_sem=o_ssem.at[b],
            recv_sem=o_rsem.at[part_of],
            device_id={"seq": b, "tp": holder},
            device_id_type=MESH,
        )

    out_local = pltpu.make_async_copy(
        fresh.at[pl.ds(seq * block, block), :],
        out_ref.at[0, :, pl.ds(pl.multiple_of(part_of * chunk, chunk), chunk)],
        o_rsem.at[part_of],
    )
    for b in range(n_seq):
        mine = jnp.logical_and(seq == b, holder == tp)

        @pl.when(mine)
        def _():
            out_local.start()

        @pl.when(jnp.logical_not(mine))
        def _():
            out_copy(b).start()

    for p in range(n_seq):
        view = out_ref.at[0, :, pl.ds(p * chunk, chunk)]
        pltpu.make_async_copy(view, view, o_rsem.at[p]).wait()

    for b in range(n_seq):

        @pl.when(jnp.logical_not(jnp.logical_and(seq == b, holder == tp)))
        def _():
            out_copy(b).wait_send()

    @pl.when(sec < n_sec - 1)
    def _():
        for j in range(n_tp):
            for k in range(n_sec):
                next_copy(j, k).wait_send()

    for d in range(1, n_tp):
        rs_copy(d).wait_send()
    for copy in part_copies:
        copy.wait_send()
    sq_copy.wait_send()
    for j in range(n_tp):

        @pl.when(jnp.logical_not(seed_is_mine(j)))
        def _():
            seed_copy(j).wait_send()


def chained(n_seq, n_sec, n_tp, token_ids, embed_columns, norm_gain, qkv_weight, out_weight):
    block = token_ids.shape[0]
    tokens = block * n_seq
    chunk = embed_columns.shape[0]
    columns = qkv_weight.shape[2]
    half = qkv_weight.shape[1]
    piece = tokens // n_sec
    groups = 4
    seq = lax.axis_index("seq")
    theirs = lax.ppermute(token_ids, "seq", [(0, 1), (1, 0)])
    every_id = jnp.where(
        seq == 0,
        jnp.concatenate([token_ids, theirs]),
        jnp.concatenate([theirs, token_ids]),
    )
    looked = pl.pallas_call(
        lookup_kernel,
        out_shape=jax.ShapeDtypeStruct((piece, chunk), jnp.bfloat16),
        in_specs=[
            pl.BlockSpec(memory_space=pltpu.SMEM),
            pl.BlockSpec(memory_space=pltpu.HBM),
        ],
        out_specs=pl.BlockSpec(memory_space=pltpu.VMEM),
        scratch_shapes=[
            pltpu.VMEM((chunk, piece * LANES), jnp.bfloat16),
            pltpu.SemaphoreType.DMA((piece,)),
        ],
    )(every_id, embed_columns)
    cosine, sine = rope_tables(jnp.arange(tokens), HEAD_WIDTH)
    cosine = jnp.concatenate([cosine, cosine], axis=1)
    sine = jnp.concatenate([-sine, sine], axis=1)
    gain = lax.dynamic_slice_in_dim(norm_gain[0], seq * half, half).astype(jnp.float32)
    gain = gain.reshape(n_tp, chunk)
    vmem = pl.BlockSpec(memory_space=pltpu.VMEM)
    hbm = pl.BlockSpec(memory_space=pltpu.HBM)
    dma = pltpu.SemaphoreType.DMA
    return pl.pallas_call(
        functools.partial(chain_kernel, n_seq, n_sec, n_tp),
        out_shape=jax.ShapeDtypeStruct((1, block, n_seq * chunk), jnp.bfloat16),
        in_specs=[vmem, vmem, vmem, vmem, hbm, hbm],
        out_specs=vmem,
        scratch_shapes=[
            pltpu.VMEM((half, columns), jnp.bfloat16),
            pltpu.VMEM((half, out_weight.shape[2]), jnp.bfloat16),
            pltpu.VMEM((n_tp, tokens, chunk), jnp.bfloat16),
            pltpu.VMEM((tokens, columns), jnp.float32),
            pltpu.VMEM((groups, tokens, columns // groups), jnp.bfloat16),
            pltpu.VMEM((groups, tokens, columns // groups), jnp.bfloat16),
            pltpu.VMEM((tokens, LANES), jnp.float32),
            pltpu.VMEM((tokens, LANES), jnp.float32),
            pltpu.VMEM((tokens, out_weight.shape[2]), jnp.bfloat16),
            pltpu.VMEM((n_tp, tokens, chunk), jnp.bfloat16),
            pltpu.VMEM((n_tp, tokens, chunk), jnp.bfloat16),
            pltpu.VMEM((tokens, chunk), jnp.bfloat16),
            dma((n_tp + 1,)),
            dma((n_sec + 1, n_tp)),
            dma((n_tp, n_sec)),
            dma((groups,)),
            dma((groups,)),
            dma,
            dma,
            dma((n_tp,)),
            dma((n_tp,)),
            dma((n_seq,)),
            dma((n_seq,)),
        ],
        compiler_params=pltpu.CompilerParams(has_side_effects=True),
    )(looked, gain, cosine, sine, qkv_weight, out_weight)


def solution(mesh):
    counts = tuple(mesh.shape[a] for a in ("seq", "section", "tp"))
    program = functools.partial(chained, *counts) if counts[0] == 2 else body
    placed = (
        P("seq"),
        P(("tp", "seq"), None),
        P("section", None),
        P("section", "seq", "tp"),
        P("section", "seq", "tp"),
    )
    return jax.shard_map(
        program, mesh=mesh, in_specs=placed, out_specs=P("section", "seq", "tp"), check_vma=False
    )
```

```python
import functools

import jax
import jax.numpy as jnp
from jax import lax
from jax.experimental import pallas as pl
from jax.experimental.pallas import tpu as pltpu
from jax.sharding import PartitionSpec as P

QUERY_HEADS = 16
KEY_VALUE_HEADS = 8
HEAD_WIDTH = 128


EPS = 1e-05
ROPE_BASE = 500000.0
MASKED = -1e30


def passed_along(value, axis, steps):
    count = lax.axis_size(axis)
    leading, last = (max(0, -steps), min(count, count - steps))
    return lax.ppermute(value, axis, [(source, source + steps) for source in range(leading, last)])


def from_root(value, axis, root):
    mine = lax.axis_index(axis) == root
    return lax.psum(jnp.where(mine, value, jnp.zeros_like(value)), axis)


def rope_tables(positions, head_size):
    half_width = head_size // 2
    inverse_freq = ROPE_BASE ** (-jnp.arange(half_width).astype(jnp.float32) * (2.0 / head_size))
    angles = positions.astype(jnp.float32)[:, None] * inverse_freq[None, :]
    return (jnp.cos(angles), jnp.sin(angles))


def rotate_half(heads, cosine_table, sine_values):
    half_width = heads.shape[-1] // 2
    first_half = heads[..., :half_width]
    second = heads[..., half_width:]
    cosine_table = cosine_table[:, None, :]
    sine_values = sine_values[:, None, :]
    return jnp.concatenate(
        [
            first_half * cosine_table - second * sine_values,
            second * cosine_table + first_half * sine_values,
        ],
        axis=-1,
    )


def norm_rows(row_block, gain_row):
    values = row_block.astype(jnp.float32)
    inverse_rms = lax.rsqrt(jnp.mean(values * values, axis=-1, keepdims=True) + EPS)
    return (values * inverse_rms * gain_row[None, :]).astype(jnp.bfloat16)


def widen(current):
    return lax.all_gather(current, "tp", axis=1, tiled=True)


def project(full_rows, gain_row, qkv_full, positions, query_heads, key_value_heads):
    row_count = full_rows.shape[0]
    normed = norm_rows(full_rows, gain_row)
    projected_rows = jnp.dot(normed, qkv_full, preferred_element_type=jnp.float32)
    projected_rows = projected_rows.reshape(
        row_count, query_heads + 2 * key_value_heads, HEAD_WIDTH
    )
    cosine_table, sine_values = rope_tables(positions, HEAD_WIDTH)
    query_rows = rotate_half(projected_rows[:, :query_heads], cosine_table, sine_values).astype(
        jnp.bfloat16
    )
    key_head_rows = rotate_half(
        projected_rows[:, query_heads : query_heads + key_value_heads], cosine_table, sine_values
    ).astype(jnp.bfloat16)
    value_head_rows = projected_rows[:, query_heads + key_value_heads :].astype(jnp.bfloat16)
    return (query_rows, key_head_rows, value_head_rows)


def attend(query_rows, key_head_rows, value_head_rows, allowed):
    row_count, query_heads, head_size = query_rows.shape
    key_value_heads = key_head_rows.shape[1]
    query_groups = query_rows.reshape(
        row_count, key_value_heads, query_heads // key_value_heads, head_size
    )
    scores = jnp.einsum(
        "rkph,ckh->kprc", query_groups, key_head_rows, preferred_element_type=jnp.float32
    ) * head_size ** (-0.5)
    scores = jnp.where(allowed[None, None], scores, MASKED)
    weights = jax.nn.softmax(scores, axis=-1).astype(jnp.bfloat16)
    attended = jnp.einsum(
        "kprc,ckh->rkph", weights, value_head_rows, preferred_element_type=jnp.float32
    )
    return attended.reshape(row_count, query_heads * head_size).astype(jnp.bfloat16)


def combine(current, attended, out_full):
    partial_value = lax.dot_general(
        attended, out_full, (((1,), (1,)), ((), ())), preferred_element_type=jnp.float32
    )
    summed = lax.psum_scatter(
        partial_value.astype(jnp.bfloat16), "tp", scatter_dimension=1, tiled=True
    ).astype(jnp.float32)
    return (current.astype(jnp.float32) + summed).astype(jnp.bfloat16)


def advance(new_rows):
    return passed_along(new_rows, "section", 1)


def body(token_ids, embed_columns, norm_gain, qkv_weight, out_weight):
    seq_count = lax.axis_size("seq")
    section_count = lax.axis_size("section")
    tensor_parallel_count = lax.axis_size("tp")
    group_index = lax.axis_index("seq")
    section_index = lax.axis_index("section")
    block_row_slice = token_ids.shape[0]
    feature_slice = embed_columns.shape[0]
    feature_cols = feature_slice * seq_count
    query_heads = QUERY_HEADS // tensor_parallel_count
    key_value_heads = KEY_VALUE_HEADS // tensor_parallel_count
    every_id = lax.all_gather(token_ids, "seq", axis=0, tiled=True)
    looked = jnp.take(embed_columns, every_id, axis=1)
    arrived = lax.all_to_all(looked, "seq", split_axis=1, concat_axis=0, tiled=True)
    residual = arrived.T
    qkv_full, out_full = (
        lax.all_gather(qkv_weight, "seq", axis=1, tiled=True),
        lax.all_gather(out_weight, "seq", axis=1, tiled=True),
    )
    qkv_full = qkv_full[0]
    out_full = out_full[0]
    gain_row = norm_gain[0].astype(jnp.float32)
    outputs = jnp.zeros((block_row_slice, feature_cols), jnp.bfloat16)
    row_ids = jnp.arange(block_row_slice)[:, None]
    column = jnp.arange(2 * block_row_slice)[None, :]
    positions = group_index * block_row_slice + jnp.arange(block_row_slice)
    allowed = jnp.where(
        column < block_row_slice, group_index > 0, column - block_row_slice <= row_ids
    )
    current = residual
    for step_number in range(section_count):
        query_rows, key_head_rows, value_head_rows = project(
            widen(current), gain_row, qkv_full, positions, query_heads, key_value_heads
        )
        anchor_heads, anchor_values = (
            from_root(key_head_rows, "seq", 0),
            from_root(value_head_rows, "seq", 0),
        )
        both_keys = jnp.concatenate([anchor_heads, key_head_rows], axis=0)
        both_values = jnp.concatenate([anchor_values, value_head_rows], axis=0)
        attended = attend(query_rows, both_keys, both_values, allowed)
        new_rows = combine(current, attended, out_full)
        outputs = jnp.where(section_index == step_number, new_rows, outputs)
        if step_number + 1 < section_count:
            current = advance(new_rows)
    return outputs[None]


LANES = 128
TOKEN_GROUP = 8
MESH = pl.DeviceIdType.MESH


def lookup_kernel(mine_ref, theirs_ref, table_ref, out_ref, tiles, sems):
    count = out_ref.shape[0]
    width = table_ref.shape[0]
    block = mine_ref.shape[0]
    first = lax.axis_index("section") * count
    ours = first // block == lax.axis_index("seq")
    ids = [
        jnp.where(ours, mine_ref[first % block + i], theirs_ref[first % block + i])
        for i in range(count)
    ]

    def fetch(i):
        start = pl.multiple_of((ids[i] // LANES) * LANES, LANES)
        return pltpu.make_async_copy(
            table_ref.at[:, pl.ds(start, LANES)], tiles.at[:, pl.ds(i * LANES, LANES)], sems.at[i]
        )

    for i in range(count):
        fetch(i).start()
    rows = lax.broadcasted_iota(jnp.int32, (LANES, LANES), 0)
    columns = lax.broadcasted_iota(jnp.int32, (LANES, LANES), 1)
    total = jnp.zeros((width, LANES), jnp.float32)
    group = min(TOKEN_GROUP, count)
    for base in range(0, count, group):
        picks = []
        for i in range(base, base + group):
            chosen = jnp.logical_and(rows == ids[i] % LANES, columns == i)
            picks.append(jnp.where(chosen, 1.0, 0.0).astype(jnp.bfloat16))
        pick = jnp.concatenate(picks, axis=0)
        for i in range(base, base + group):
            fetch(i).wait()
        total += jnp.dot(
            tiles[:, base * LANES : (base + group) * LANES], pick, preferred_element_type=jnp.float32
        )
    out_ref[...] = total.T[:count].astype(jnp.bfloat16)


def chain_kernel(
    n_seq,
    n_sec,
    n_tp,
    piece_ref,
    gain_ref,
    cos_ref,
    sin_ref,
    qkv_ref,
    outw_ref,
    out_ref,
    wq,
    wo,
    hidden,
    acc,
    part_send,
    part_recv,
    sq_send,
    sq_recv,
    kept,
    heads,
    rs_send,
    rs_recv,
    fresh,
    w_sem,
    h_ssem,
    h_rsem,
    p_ssem,
    p_rsem,
    q_ssem,
    q_rsem,
    r_ssem,
    r_rsem,
    o_ssem,
    o_rsem,
):
    seq, sec, tp = (lax.axis_index(a) for a in ("seq", "section", "tp"))
    tokens, chunk = fresh.shape
    piece = tokens // n_sec
    block = out_ref.shape[1]
    _, groups, _, group_width = part_send.shape
    query_heads = QUERY_HEADS // n_tp
    kv_heads = KEY_VALUE_HEADS // n_tp

    load_q = [
        pltpu.make_async_copy(
            qkv_ref.at[0, pl.ds(((tp + d) % n_tp) * chunk, chunk), :],
            wq.at[pl.ds(((tp + d) % n_tp) * chunk, chunk), :],
            w_sem.at[d],
        )
        for d in range(n_tp)
    ]
    load_o = pltpu.make_async_copy(outw_ref.at[0], wo, w_sem.at[n_tp])
    for c in load_q:
        c.start()
    load_o.start()

    shard = tp * n_seq + seq
    half, slot = shard // n_tp, shard % n_tp

    def seed_copy(j):
        return pltpu.make_async_remote_copy(
            src_ref=piece_ref,
            dst_ref=hidden.at[slot, pl.ds(sec * piece, piece), :],
            send_sem=h_ssem.at[0, j],
            recv_sem=h_rsem.at[slot, sec],
            device_id={"seq": half, "section": 0, "tp": j},
            device_id_type=MESH,
        )

    def seed_is_mine(j):
        return jnp.logical_and(sec == 0, jnp.logical_and(half == seq, tp == j))

    seed_local = pltpu.make_async_copy(
        piece_ref, hidden.at[slot, pl.ds(sec * piece, piece), :], h_rsem.at[slot, sec]
    )
    for j in range(n_tp):
        mine = seed_is_mine(j)

        @pl.when(mine)
        def _():
            seed_local.start()

        @pl.when(jnp.logical_not(mine))
        def _():
            seed_copy(j).start()

    other = 1 - seq
    pieces = block // piece

    def square_copy(p):
        return pltpu.make_async_remote_copy(
            src_ref=sq_send.at[p],
            dst_ref=sq_recv.at[p],
            send_sem=q_ssem.at[p],
            recv_sem=q_rsem.at[p],
            device_id={"seq": other},
            device_id_type=MESH,
        )

    def part_copy(p, g):
        return pltpu.make_async_remote_copy(
            src_ref=part_send.at[p, g],
            dst_ref=part_recv.at[p, g],
            send_sem=p_ssem.at[p, g],
            recv_sem=p_rsem.at[p, g],
            device_id={"seq": other},
            device_id_type=MESH,
        )

    def rs_copy(p, d):
        return pltpu.make_async_remote_copy(
            src_ref=rs_send.at[p, d],
            dst_ref=rs_recv.at[p, d],
            send_sem=r_ssem.at[p, d],
            recv_sem=r_rsem.at[p, d],
            device_id={"tp": (tp + d) % n_tp},
            device_id_type=MESH,
        )

    def next_copy(d, k):
        return pltpu.make_async_remote_copy(
            src_ref=fresh.at[pl.ds(k * piece, piece), :],
            dst_ref=hidden.at[tp, pl.ds(k * piece, piece), :],
            send_sem=h_ssem.at[k + 1, d],
            recv_sem=h_rsem.at[tp, k],
            device_id={"section": sec + 1, "tp": (tp + n_tp - d) % n_tp},
            device_id_type=MESH,
        )

    place = seq * n_tp + tp
    holder, part_of = place // n_seq, place % n_seq

    def out_copy(b):
        return pltpu.make_async_remote_copy(
            src_ref=fresh.at[pl.ds(b * block, block), :],
            dst_ref=out_ref.at[0, :, pl.ds(pl.multiple_of(part_of * chunk, chunk), chunk)],
            send_sem=o_ssem.at[b],
            recv_sem=o_rsem.at[part_of],
            device_id={"seq": b, "tp": holder},
            device_id_type=MESH,
        )

    def project(p):
        span = slice(p * block, (p + 1) * block)
        squares = jnp.zeros((block, LANES), jnp.float32)
        for d in range(n_tp):
            c = (tp + d) % n_tp
            for k in range(p * pieces, (p + 1) * pieces):
                view = hidden.at[c, pl.ds(k * piece, piece), :]
                pltpu.make_async_copy(view, view, h_rsem.at[c, k]).wait()
            if p == 0:
                load_q[d].wait()
            rows = hidden[c, span, :].astype(jnp.float32)
            sq = rows * rows
            for k in range(chunk // LANES):
                squares += sq[:, k * LANES : (k + 1) * LANES]
            at = pl.multiple_of(seq * (n_tp * chunk) + c * chunk, chunk)
            gain = gain_ref[:, pl.ds(at, chunk)].astype(jnp.float32)
            scaled = (rows * gain).astype(jnp.bfloat16)
            if d == n_tp - 1:
                sq_send[p] = squares
                square_copy(p).start()
            for g in range(groups):
                cols = slice(g * group_width, (g + 1) * group_width)
                product = jnp.dot(
                    scaled,
                    wq[pl.ds(pl.multiple_of(c * chunk, chunk), chunk), cols],
                    preferred_element_type=jnp.float32,
                )
                if d > 0:
                    product += acc[span, cols]
                acc[span, cols] = product
                if d == n_tp - 1:
                    part_send[p, g] = product.astype(jnp.bfloat16)
                    part_copy(p, g).start()

    repeat = query_heads // kv_heads

    def attend_block(p):
        span = slice(p * block, (p + 1) * block)
        square_copy(p).wait_recv()
        features = n_seq * n_tp * chunk
        mean = jnp.sum(sq_send[p] + sq_recv[p], axis=-1, keepdims=True) * (1.0 / features)
        inverse_rms = lax.rsqrt(mean + EPS)
        cosine, sine = cos_ref[span, :], sin_ref[span, :]
        ready = []
        for g in range(groups):
            part_copy(p, g).wait_recv()
            cols = slice(g * group_width, (g + 1) * group_width)
            whole = (acc[span, cols] + part_recv[p, g].astype(jnp.float32)) * inverse_rms
            for k in range(group_width // HEAD_WIDTH):
                head = whole[:, k * HEAD_WIDTH : (k + 1) * HEAD_WIDTH]
                if len(ready) < query_heads + kv_heads:
                    head = head * cosine + pltpu.roll(head, HEAD_WIDTH // 2, 1) * sine
                head = head.astype(jnp.bfloat16)
                if len(ready) >= query_heads:
                    kept[len(ready) - query_heads, span, :] = head
                ready.append(head)
        known = (p + 1) * block
        row_at = lax.broadcasted_iota(jnp.int32, (repeat, block, known), 1)
        key_at = lax.broadcasted_iota(jnp.int32, (repeat, block, known), 2)
        visible = (key_at <= row_at + p * block).reshape(repeat * block, known)
        for h in range(kv_heads):
            queries = jnp.concatenate(ready[h * repeat : (h + 1) * repeat], axis=0)
            scores = lax.dot_general(
                queries, kept[h, :known, :], (((1,), (1,)), ((), ())), preferred_element_type=jnp.float32
            ) * HEAD_WIDTH ** (-0.5)
            scores = jnp.where(visible, scores, MASKED)
            shifted = jnp.exp(scores - jnp.max(scores, axis=-1, keepdims=True))
            weights = (shifted / jnp.sum(shifted, axis=-1, keepdims=True)).astype(jnp.bfloat16)
            attended = jnp.dot(
                weights, kept[kv_heads + h, :known, :], preferred_element_type=jnp.float32
            ).astype(jnp.bfloat16)
            for r in range(repeat):
                at = (h * repeat + r) * HEAD_WIDTH
                heads[span, at : at + HEAD_WIDTH] = attended[r * block : (r + 1) * block]
        if p == 0:
            load_o.wait()
        attended = heads[span, :]
        for d in [*range(1, n_tp), 0]:
            c = (tp + d) % n_tp
            partial = lax.dot_general(
                attended,
                wo[pl.ds(pl.multiple_of(c * chunk, chunk), chunk), :],
                (((1,), (1,)), ((), ())),
                preferred_element_type=jnp.float32,
            ).astype(jnp.bfloat16)
            rs_send[p, d] = partial
            if d:
                rs_copy(p, d).start()

    def forward(p):
        span = slice(p * block, (p + 1) * block)
        summed = rs_send[p, 0].astype(jnp.float32)
        for d in range(1, n_tp):
            rs_copy(p, d).wait_recv()
            summed += rs_recv[p, d].astype(jnp.float32)
        fresh[span, :] = (hidden[tp, span, :].astype(jnp.float32) + summed).astype(jnp.bfloat16)

        @pl.when(sec < n_sec - 1)
        def _():
            for d in range(n_tp):
                for k in range(p * pieces, (p + 1) * pieces):
                    next_copy(d, k).start()

        mine = jnp.logical_and(seq == p, holder == tp)

        @pl.when(mine)
        def _():
            pltpu.make_async_copy(
                fresh.at[pl.ds(seq * block, block), :],
                out_ref.at[0, :, pl.ds(pl.multiple_of(part_of * chunk, chunk), chunk)],
                o_rsem.at[part_of],
            ).start()

        @pl.when(jnp.logical_not(mine))
        def _():
            out_copy(p).start()

    project(0)
    attend_block(0)
    project(1)
    forward(0)
    attend_block(1)
    forward(1)

    for p in range(n_seq):
        view = out_ref.at[0, :, pl.ds(p * chunk, chunk)]
        pltpu.make_async_copy(view, view, o_rsem.at[p]).wait()

    for p in range(n_seq):

        @pl.when(jnp.logical_not(jnp.logical_and(seq == p, holder == tp)))
        def _():
            out_copy(p).wait_send()

    @pl.when(sec < n_sec - 1)
    def _():
        for d in range(n_tp):
            for k in range(n_sec):
                next_copy(d, k).wait_send()

    for p in range(n_seq):
        for d in range(1, n_tp):
            rs_copy(p, d).wait_send()
        for g in range(groups):
            part_copy(p, g).wait_send()
        square_copy(p).wait_send()
    for j in range(n_tp):

        @pl.when(jnp.logical_not(seed_is_mine(j)))
        def _():
            seed_copy(j).wait_send()


def chained(n_seq, n_sec, n_tp, token_ids, embed_columns, norm_gain, qkv_weight, out_weight):
    block = token_ids.shape[0]
    tokens = block * n_seq
    chunk = embed_columns.shape[0]
    columns = qkv_weight.shape[2]
    half = qkv_weight.shape[1]
    piece = tokens // n_sec
    groups = 4
    theirs = lax.ppermute(token_ids, "seq", [(0, 1), (1, 0)])
    looked = pl.pallas_call(
        lookup_kernel,
        out_shape=jax.ShapeDtypeStruct((piece, chunk), jnp.bfloat16),
        in_specs=[
            pl.BlockSpec(memory_space=pltpu.SMEM),
            pl.BlockSpec(memory_space=pltpu.SMEM),
            pl.BlockSpec(memory_space=pltpu.HBM),
        ],
        out_specs=pl.BlockSpec(memory_space=pltpu.VMEM),
        scratch_shapes=[
            pltpu.VMEM((chunk, piece * LANES), jnp.bfloat16),
            pltpu.SemaphoreType.DMA((piece,)),
        ],
    )(token_ids, theirs, embed_columns)
    cosine, sine = rope_tables(jnp.arange(tokens), HEAD_WIDTH)
    cosine = jnp.concatenate([cosine, cosine], axis=1)
    sine = jnp.concatenate([-sine, sine], axis=1)
    vmem = pl.BlockSpec(memory_space=pltpu.VMEM)
    hbm = pl.BlockSpec(memory_space=pltpu.HBM)
    dma = pltpu.SemaphoreType.DMA
    return pl.pallas_call(
        functools.partial(chain_kernel, n_seq, n_sec, n_tp),
        out_shape=jax.ShapeDtypeStruct((1, block, n_seq * chunk), jnp.bfloat16),
        in_specs=[vmem, vmem, vmem, vmem, hbm, hbm],
        out_specs=vmem,
        scratch_shapes=[
            pltpu.VMEM((half, columns), jnp.bfloat16),
            pltpu.VMEM((half, out_weight.shape[2]), jnp.bfloat16),
            pltpu.VMEM((n_tp, tokens, chunk), jnp.bfloat16),
            pltpu.VMEM((tokens, columns), jnp.float32),
            pltpu.VMEM((n_seq, groups, block, columns // groups), jnp.bfloat16),
            pltpu.VMEM((n_seq, groups, block, columns // groups), jnp.bfloat16),
            pltpu.VMEM((n_seq, block, LANES), jnp.float32),
            pltpu.VMEM((n_seq, block, LANES), jnp.float32),
            pltpu.VMEM((2 * KEY_VALUE_HEADS // n_tp, tokens, HEAD_WIDTH), jnp.bfloat16),
            pltpu.VMEM((tokens, out_weight.shape[2]), jnp.bfloat16),
            pltpu.VMEM((n_seq, n_tp, block, chunk), jnp.bfloat16),
            pltpu.VMEM((n_seq, n_tp, block, chunk), jnp.bfloat16),
            pltpu.VMEM((tokens, chunk), jnp.bfloat16),
            dma((n_tp + 1,)),
            dma((n_sec + 1, n_tp)),
            dma((n_tp, n_sec)),
            dma((n_seq, groups)),
            dma((n_seq, groups)),
            dma((n_seq,)),
            dma((n_seq,)),
            dma((n_seq, n_tp)),
            dma((n_seq, n_tp)),
            dma((n_seq,)),
            dma((n_seq,)),
        ],
        compiler_params=pltpu.CompilerParams(has_side_effects=True),
    )(looked, norm_gain, cosine, sine, qkv_weight, out_weight)


def solution(mesh):
    counts = tuple(mesh.shape[a] for a in ("seq", "section", "tp"))
    program = functools.partial(chained, *counts) if counts[0] == 2 else body
    placed = (
        P("seq"),
        P(("tp", "seq"), None),
        P("section", None),
        P("section", "seq", "tp"),
        P("section", "seq", "tp"),
    )
    return jax.shard_map(
        program, mesh=mesh, in_specs=placed, out_specs=P("section", "seq", "tp"), check_vma=False
    )
```

```python
import functools

import jax
import jax.numpy as jnp
from jax import lax
from jax.experimental import pallas as pl
from jax.experimental.pallas import tpu as pltpu
from jax.sharding import PartitionSpec as P

QUERY_HEADS = 16
KEY_VALUE_HEADS = 8
HEAD_WIDTH = 128


EPS = 1e-05
ROPE_BASE = 500000.0
MASKED = -1e30


def passed_along(value, axis, steps):
    count = lax.axis_size(axis)
    leading, last = (max(0, -steps), min(count, count - steps))
    return lax.ppermute(value, axis, [(source, source + steps) for source in range(leading, last)])


def from_root(value, axis, root):
    mine = lax.axis_index(axis) == root
    return lax.psum(jnp.where(mine, value, jnp.zeros_like(value)), axis)


def rope_tables(positions, head_size):
    half_width = head_size // 2
    inverse_freq = ROPE_BASE ** (-jnp.arange(half_width).astype(jnp.float32) * (2.0 / head_size))
    angles = positions.astype(jnp.float32)[:, None] * inverse_freq[None, :]
    return (jnp.cos(angles), jnp.sin(angles))


def rotate_half(heads, cosine_table, sine_values):
    half_width = heads.shape[-1] // 2
    first_half = heads[..., :half_width]
    second = heads[..., half_width:]
    cosine_table = cosine_table[:, None, :]
    sine_values = sine_values[:, None, :]
    return jnp.concatenate(
        [
            first_half * cosine_table - second * sine_values,
            second * cosine_table + first_half * sine_values,
        ],
        axis=-1,
    )


def norm_rows(row_block, gain_row):
    values = row_block.astype(jnp.float32)
    inverse_rms = lax.rsqrt(jnp.mean(values * values, axis=-1, keepdims=True) + EPS)
    return (values * inverse_rms * gain_row[None, :]).astype(jnp.bfloat16)


def widen(current):
    return lax.all_gather(current, "tp", axis=1, tiled=True)


def project(full_rows, gain_row, qkv_full, positions, query_heads, key_value_heads):
    row_count = full_rows.shape[0]
    normed = norm_rows(full_rows, gain_row)
    projected_rows = jnp.dot(normed, qkv_full, preferred_element_type=jnp.float32)
    projected_rows = projected_rows.reshape(
        row_count, query_heads + 2 * key_value_heads, HEAD_WIDTH
    )
    cosine_table, sine_values = rope_tables(positions, HEAD_WIDTH)
    query_rows = rotate_half(projected_rows[:, :query_heads], cosine_table, sine_values).astype(
        jnp.bfloat16
    )
    key_head_rows = rotate_half(
        projected_rows[:, query_heads : query_heads + key_value_heads], cosine_table, sine_values
    ).astype(jnp.bfloat16)
    value_head_rows = projected_rows[:, query_heads + key_value_heads :].astype(jnp.bfloat16)
    return (query_rows, key_head_rows, value_head_rows)


def attend(query_rows, key_head_rows, value_head_rows, allowed):
    row_count, query_heads, head_size = query_rows.shape
    key_value_heads = key_head_rows.shape[1]
    query_groups = query_rows.reshape(
        row_count, key_value_heads, query_heads // key_value_heads, head_size
    )
    scores = jnp.einsum(
        "rkph,ckh->kprc", query_groups, key_head_rows, preferred_element_type=jnp.float32
    ) * head_size ** (-0.5)
    scores = jnp.where(allowed[None, None], scores, MASKED)
    weights = jax.nn.softmax(scores, axis=-1).astype(jnp.bfloat16)
    attended = jnp.einsum(
        "kprc,ckh->rkph", weights, value_head_rows, preferred_element_type=jnp.float32
    )
    return attended.reshape(row_count, query_heads * head_size).astype(jnp.bfloat16)


def combine(current, attended, out_full):
    partial_value = lax.dot_general(
        attended, out_full, (((1,), (1,)), ((), ())), preferred_element_type=jnp.float32
    )
    summed = lax.psum_scatter(
        partial_value.astype(jnp.bfloat16), "tp", scatter_dimension=1, tiled=True
    ).astype(jnp.float32)
    return (current.astype(jnp.float32) + summed).astype(jnp.bfloat16)


def advance(new_rows):
    return passed_along(new_rows, "section", 1)


def body(token_ids, embed_columns, norm_gain, qkv_weight, out_weight):
    seq_count = lax.axis_size("seq")
    section_count = lax.axis_size("section")
    tensor_parallel_count = lax.axis_size("tp")
    group_index = lax.axis_index("seq")
    section_index = lax.axis_index("section")
    block_row_slice = token_ids.shape[0]
    feature_slice = embed_columns.shape[0]
    feature_cols = feature_slice * seq_count
    query_heads = QUERY_HEADS // tensor_parallel_count
    key_value_heads = KEY_VALUE_HEADS // tensor_parallel_count
    every_id = lax.all_gather(token_ids, "seq", axis=0, tiled=True)
    looked = jnp.take(embed_columns, every_id, axis=1)
    arrived = lax.all_to_all(looked, "seq", split_axis=1, concat_axis=0, tiled=True)
    residual = arrived.T
    qkv_full, out_full = (
        lax.all_gather(qkv_weight, "seq", axis=1, tiled=True),
        lax.all_gather(out_weight, "seq", axis=1, tiled=True),
    )
    qkv_full = qkv_full[0]
    out_full = out_full[0]
    gain_row = norm_gain[0].astype(jnp.float32)
    outputs = jnp.zeros((block_row_slice, feature_cols), jnp.bfloat16)
    row_ids = jnp.arange(block_row_slice)[:, None]
    column = jnp.arange(2 * block_row_slice)[None, :]
    positions = group_index * block_row_slice + jnp.arange(block_row_slice)
    allowed = jnp.where(
        column < block_row_slice, group_index > 0, column - block_row_slice <= row_ids
    )
    current = residual
    for step_number in range(section_count):
        query_rows, key_head_rows, value_head_rows = project(
            widen(current), gain_row, qkv_full, positions, query_heads, key_value_heads
        )
        anchor_heads, anchor_values = (
            from_root(key_head_rows, "seq", 0),
            from_root(value_head_rows, "seq", 0),
        )
        both_keys = jnp.concatenate([anchor_heads, key_head_rows], axis=0)
        both_values = jnp.concatenate([anchor_values, value_head_rows], axis=0)
        attended = attend(query_rows, both_keys, both_values, allowed)
        new_rows = combine(current, attended, out_full)
        outputs = jnp.where(section_index == step_number, new_rows, outputs)
        if step_number + 1 < section_count:
            current = advance(new_rows)
    return outputs[None]


LANES = 128
TOKEN_GROUP = 8
MESH = pl.DeviceIdType.MESH


def lookup_kernel(mine_ref, theirs_ref, table_ref, out_ref, tiles, sems):
    count = out_ref.shape[0]
    width = table_ref.shape[0]
    block = mine_ref.shape[0]
    first = lax.axis_index("section") * count
    ours = first // block == lax.axis_index("seq")
    ids = [
        jnp.where(ours, mine_ref[first % block + i], theirs_ref[first % block + i])
        for i in range(count)
    ]

    def fetch(i):
        start = pl.multiple_of((ids[i] // LANES) * LANES, LANES)
        return pltpu.make_async_copy(
            table_ref.at[:, pl.ds(start, LANES)], tiles.at[:, pl.ds(i * LANES, LANES)], sems.at[i]
        )

    for i in range(count):
        fetch(i).start()
    rows = lax.broadcasted_iota(jnp.int32, (LANES, LANES), 0)
    columns = lax.broadcasted_iota(jnp.int32, (LANES, LANES), 1)
    total = jnp.zeros((width, LANES), jnp.float32)
    group = min(TOKEN_GROUP, count)
    for base in range(0, count, group):
        picks = []
        for i in range(base, base + group):
            chosen = jnp.logical_and(rows == ids[i] % LANES, columns == i)
            picks.append(jnp.where(chosen, 1.0, 0.0).astype(jnp.bfloat16))
        pick = jnp.concatenate(picks, axis=0)
        for i in range(base, base + group):
            fetch(i).wait()
        total += jnp.dot(
            tiles[:, base * LANES : (base + group) * LANES], pick, preferred_element_type=jnp.float32
        )
    out_ref[...] = total.T[:count].astype(jnp.bfloat16)


def chain_kernel(
    n_seq,
    n_sec,
    n_tp,
    piece_ref,
    gain_ref,
    cos_ref,
    sin_ref,
    qkv_ref,
    outw_ref,
    out_ref,
    wq,
    wo,
    hidden,
    acc,
    part_send,
    part_recv,
    sq_send,
    sq_recv,
    kept,
    heads,
    rs_send,
    rs_recv,
    fresh,
    relay,
    a_ssem,
    a_rsem,
    w_sem,
    h_ssem,
    h_rsem,
    p_ssem,
    p_rsem,
    q_ssem,
    q_rsem,
    r_ssem,
    r_rsem,
    o_ssem,
    o_rsem,
):
    seq, sec, tp = (lax.axis_index(a) for a in ("seq", "section", "tp"))
    tokens, chunk = fresh.shape
    piece = tokens // n_sec
    block = out_ref.shape[1]
    _, groups, _, group_width = part_send.shape
    query_heads = QUERY_HEADS // n_tp
    kv_heads = KEY_VALUE_HEADS // n_tp

    load_q = [
        pltpu.make_async_copy(
            qkv_ref.at[0, pl.ds(((tp + d) % n_tp) * chunk, chunk), :],
            wq.at[pl.ds(((tp + d) % n_tp) * chunk, chunk), :],
            w_sem.at[d],
        )
        for d in range(n_tp)
    ]
    load_o = pltpu.make_async_copy(outw_ref.at[0], wo, w_sem.at[n_tp])
    for c in load_q:
        c.start()
    load_o.start()

    def spread_copy(d):
        return pltpu.make_async_remote_copy(
            src_ref=piece_ref,
            dst_ref=relay.at[tp],
            send_sem=a_ssem.at[d],
            recv_sem=a_rsem.at[tp],
            device_id={"tp": (tp + d) % n_tp},
            device_id_type=MESH,
        )

    def seed(d):
        source = (tp + n_tp - d) % n_tp
        shard = source * n_seq + seq
        half, slot = shard // n_tp, shard % n_tp
        held = relay.at[source] if d else piece_ref
        target = hidden.at[slot, pl.ds(sec * piece, piece), :]
        mine = jnp.logical_and(sec == 0, half == seq)
        local = pltpu.make_async_copy(held, target, h_rsem.at[slot, sec])
        remote = pltpu.make_async_remote_copy(
            src_ref=held,
            dst_ref=target,
            send_sem=h_ssem.at[0, d],
            recv_sem=h_rsem.at[slot, sec],
            device_id={"seq": half, "section": 0},
            device_id_type=MESH,
        )
        return source, mine, local, remote

    for d in range(1, n_tp):
        spread_copy(d).start()
    for d in range(n_tp):
        source, mine, local, remote = seed(d)
        if d:
            pltpu.make_async_copy(relay.at[source], relay.at[source], a_rsem.at[source]).wait()

        @pl.when(mine)
        def _():
            local.start()

        @pl.when(jnp.logical_not(mine))
        def _():
            remote.start()

    other = 1 - seq
    pieces = block // piece

    def square_copy(p):
        return pltpu.make_async_remote_copy(
            src_ref=sq_send.at[p],
            dst_ref=sq_recv.at[p],
            send_sem=q_ssem.at[p],
            recv_sem=q_rsem.at[p],
            device_id={"seq": other},
            device_id_type=MESH,
        )

    def part_copy(p, g):
        return pltpu.make_async_remote_copy(
            src_ref=part_send.at[p, g],
            dst_ref=part_recv.at[p, g],
            send_sem=p_ssem.at[p, g],
            recv_sem=p_rsem.at[p, g],
            device_id={"seq": other},
            device_id_type=MESH,
        )

    def rs_copy(p, d):
        return pltpu.make_async_remote_copy(
            src_ref=rs_send.at[p, d],
            dst_ref=rs_recv.at[p, d],
            send_sem=r_ssem.at[p, d],
            recv_sem=r_rsem.at[p, d],
            device_id={"tp": (tp + d) % n_tp},
            device_id_type=MESH,
        )

    def next_copy(d, k):
        return pltpu.make_async_remote_copy(
            src_ref=fresh.at[pl.ds(k * piece, piece), :],
            dst_ref=hidden.at[tp, pl.ds(k * piece, piece), :],
            send_sem=h_ssem.at[k + 1, d],
            recv_sem=h_rsem.at[tp, k],
            device_id={"section": sec + 1, "tp": (tp + n_tp - d) % n_tp},
            device_id_type=MESH,
        )

    place = seq * n_tp + tp
    holder, part_of = place // n_seq, place % n_seq

    def out_copy(b):
        return pltpu.make_async_remote_copy(
            src_ref=fresh.at[pl.ds(b * block, block), :],
            dst_ref=out_ref.at[0, :, pl.ds(pl.multiple_of(part_of * chunk, chunk), chunk)],
            send_sem=o_ssem.at[b],
            recv_sem=o_rsem.at[part_of],
            device_id={"seq": b, "tp": holder},
            device_id_type=MESH,
        )

    def project(p):
        span = slice(p * block, (p + 1) * block)
        squares = jnp.zeros((block, LANES), jnp.float32)
        for d in range(n_tp):
            c = (tp + d) % n_tp
            for k in range(p * pieces, (p + 1) * pieces):
                view = hidden.at[c, pl.ds(k * piece, piece), :]
                pltpu.make_async_copy(view, view, h_rsem.at[c, k]).wait()
            if p == 0:
                load_q[d].wait()
            rows = hidden[c, span, :].astype(jnp.float32)
            sq = rows * rows
            for k in range(chunk // LANES):
                squares += sq[:, k * LANES : (k + 1) * LANES]
            at = pl.multiple_of(seq * (n_tp * chunk) + c * chunk, chunk)
            gain = gain_ref[:, pl.ds(at, chunk)].astype(jnp.float32)
            scaled = (rows * gain).astype(jnp.bfloat16)
            if d == n_tp - 1:
                sq_send[p] = squares
                square_copy(p).start()
            for g in range(groups):
                cols = slice(g * group_width, (g + 1) * group_width)
                product = jnp.dot(
                    scaled,
                    wq[pl.ds(pl.multiple_of(c * chunk, chunk), chunk), cols],
                    preferred_element_type=jnp.float32,
                )
                if d > 0:
                    product += acc[span, cols]
                acc[span, cols] = product
                if d == n_tp - 1:
                    part_send[p, g] = product.astype(jnp.bfloat16)
                    part_copy(p, g).start()

    repeat = query_heads // kv_heads

    def attend_block(p):
        span = slice(p * block, (p + 1) * block)
        square_copy(p).wait_recv()
        features = n_seq * n_tp * chunk
        mean = jnp.sum(sq_send[p] + sq_recv[p], axis=-1, keepdims=True) * (1.0 / features)
        inverse_rms = lax.rsqrt(mean + EPS)
        cosine, sine = cos_ref[span, :], sin_ref[span, :]
        ready = []
        for g in range(groups):
            part_copy(p, g).wait_recv()
            cols = slice(g * group_width, (g + 1) * group_width)
            whole = (acc[span, cols] + part_recv[p, g].astype(jnp.float32)) * inverse_rms
            for k in range(group_width // HEAD_WIDTH):
                head = whole[:, k * HEAD_WIDTH : (k + 1) * HEAD_WIDTH]
                if len(ready) < query_heads + kv_heads:
                    head = head * cosine + pltpu.roll(head, HEAD_WIDTH // 2, 1) * sine
                head = head.astype(jnp.bfloat16)
                if len(ready) >= query_heads:
                    kept[len(ready) - query_heads, span, :] = head
                ready.append(head)
        known = (p + 1) * block
        row_at = lax.broadcasted_iota(jnp.int32, (repeat, block, known), 1)
        key_at = lax.broadcasted_iota(jnp.int32, (repeat, block, known), 2)
        visible = (key_at <= row_at + p * block).reshape(repeat * block, known)
        for h in range(kv_heads):
            queries = jnp.concatenate(ready[h * repeat : (h + 1) * repeat], axis=0)
            scores = lax.dot_general(
                queries, kept[h, :known, :], (((1,), (1,)), ((), ())), preferred_element_type=jnp.float32
            ) * HEAD_WIDTH ** (-0.5)
            scores = jnp.where(visible, scores, MASKED)
            shifted = jnp.exp(scores - jnp.max(scores, axis=-1, keepdims=True))
            weights = (shifted / jnp.sum(shifted, axis=-1, keepdims=True)).astype(jnp.bfloat16)
            attended = jnp.dot(
                weights, kept[kv_heads + h, :known, :], preferred_element_type=jnp.float32
            ).astype(jnp.bfloat16)
            for r in range(repeat):
                at = (h * repeat + r) * HEAD_WIDTH
                heads[span, at : at + HEAD_WIDTH] = attended[r * block : (r + 1) * block]
        if p == 0:
            load_o.wait()
        attended = heads[span, :]
        for d in [*range(1, n_tp), 0]:
            c = (tp + d) % n_tp
            partial = lax.dot_general(
                attended,
                wo[pl.ds(pl.multiple_of(c * chunk, chunk), chunk), :],
                (((1,), (1,)), ((), ())),
                preferred_element_type=jnp.float32,
            ).astype(jnp.bfloat16)
            rs_send[p, d] = partial
            if d:
                rs_copy(p, d).start()

    def forward(p):
        span = slice(p * block, (p + 1) * block)
        summed = rs_send[p, 0].astype(jnp.float32)
        for d in range(1, n_tp):
            rs_copy(p, d).wait_recv()
            summed += rs_recv[p, d].astype(jnp.float32)
        fresh[span, :] = (hidden[tp, span, :].astype(jnp.float32) + summed).astype(jnp.bfloat16)

        @pl.when(sec < n_sec - 1)
        def _():
            for d in range(n_tp):
                for k in range(p * pieces, (p + 1) * pieces):
                    next_copy(d, k).start()

        mine = jnp.logical_and(seq == p, holder == tp)

        @pl.when(mine)
        def _():
            pltpu.make_async_copy(
                fresh.at[pl.ds(seq * block, block), :],
                out_ref.at[0, :, pl.ds(pl.multiple_of(part_of * chunk, chunk), chunk)],
                o_rsem.at[part_of],
            ).start()

        @pl.when(jnp.logical_not(mine))
        def _():
            out_copy(p).start()

    project(0)
    attend_block(0)
    project(1)
    forward(0)
    attend_block(1)
    forward(1)

    for p in range(n_seq):
        view = out_ref.at[0, :, pl.ds(p * chunk, chunk)]
        pltpu.make_async_copy(view, view, o_rsem.at[p]).wait()

    for p in range(n_seq):

        @pl.when(jnp.logical_not(jnp.logical_and(seq == p, holder == tp)))
        def _():
            out_copy(p).wait_send()

    @pl.when(sec < n_sec - 1)
    def _():
        for d in range(n_tp):
            for k in range(n_sec):
                next_copy(d, k).wait_send()

    for p in range(n_seq):
        for d in range(1, n_tp):
            rs_copy(p, d).wait_send()
        for g in range(groups):
            part_copy(p, g).wait_send()
        square_copy(p).wait_send()
    for d in range(n_tp):
        _, mine, _, remote = seed(d)

        @pl.when(jnp.logical_not(mine))
        def _():
            remote.wait_send()

        if d:
            spread_copy(d).wait_send()


def chained(n_seq, n_sec, n_tp, token_ids, embed_columns, norm_gain, qkv_weight, out_weight):
    block = token_ids.shape[0]
    tokens = block * n_seq
    chunk = embed_columns.shape[0]
    columns = qkv_weight.shape[2]
    half = qkv_weight.shape[1]
    piece = tokens // n_sec
    groups = 4
    theirs = lax.ppermute(token_ids, "seq", [(0, 1), (1, 0)])
    looked = pl.pallas_call(
        lookup_kernel,
        out_shape=jax.ShapeDtypeStruct((piece, chunk), jnp.bfloat16),
        in_specs=[
            pl.BlockSpec(memory_space=pltpu.SMEM),
            pl.BlockSpec(memory_space=pltpu.SMEM),
            pl.BlockSpec(memory_space=pltpu.HBM),
        ],
        out_specs=pl.BlockSpec(memory_space=pltpu.VMEM),
        scratch_shapes=[
            pltpu.VMEM((chunk, piece * LANES), jnp.bfloat16),
            pltpu.SemaphoreType.DMA((piece,)),
        ],
    )(token_ids, theirs, embed_columns)
    cosine, sine = rope_tables(jnp.arange(tokens), HEAD_WIDTH)
    cosine = jnp.concatenate([cosine, cosine], axis=1)
    sine = jnp.concatenate([-sine, sine], axis=1)
    vmem = pl.BlockSpec(memory_space=pltpu.VMEM)
    hbm = pl.BlockSpec(memory_space=pltpu.HBM)
    dma = pltpu.SemaphoreType.DMA
    return pl.pallas_call(
        functools.partial(chain_kernel, n_seq, n_sec, n_tp),
        out_shape=jax.ShapeDtypeStruct((1, block, n_seq * chunk), jnp.bfloat16),
        in_specs=[vmem, vmem, vmem, vmem, hbm, hbm],
        out_specs=vmem,
        scratch_shapes=[
            pltpu.VMEM((half, columns), jnp.bfloat16),
            pltpu.VMEM((half, out_weight.shape[2]), jnp.bfloat16),
            pltpu.VMEM((n_tp, tokens, chunk), jnp.bfloat16),
            pltpu.VMEM((tokens, columns), jnp.float32),
            pltpu.VMEM((n_seq, groups, block, columns // groups), jnp.bfloat16),
            pltpu.VMEM((n_seq, groups, block, columns // groups), jnp.bfloat16),
            pltpu.VMEM((n_seq, block, LANES), jnp.float32),
            pltpu.VMEM((n_seq, block, LANES), jnp.float32),
            pltpu.VMEM((2 * KEY_VALUE_HEADS // n_tp, tokens, HEAD_WIDTH), jnp.bfloat16),
            pltpu.VMEM((tokens, out_weight.shape[2]), jnp.bfloat16),
            pltpu.VMEM((n_seq, n_tp, block, chunk), jnp.bfloat16),
            pltpu.VMEM((n_seq, n_tp, block, chunk), jnp.bfloat16),
            pltpu.VMEM((tokens, chunk), jnp.bfloat16),
            pltpu.VMEM((n_tp, piece, chunk), jnp.bfloat16),
            dma((n_tp,)),
            dma((n_tp,)),
            dma((n_tp + 1,)),
            dma((n_sec + 1, n_tp)),
            dma((n_tp, n_sec)),
            dma((n_seq, groups)),
            dma((n_seq, groups)),
            dma((n_seq,)),
            dma((n_seq,)),
            dma((n_seq, n_tp)),
            dma((n_seq, n_tp)),
            dma((n_seq,)),
            dma((n_seq,)),
        ],
        compiler_params=pltpu.CompilerParams(has_side_effects=True),
    )(looked, norm_gain, cosine, sine, qkv_weight, out_weight)


def solution(mesh):
    counts = tuple(mesh.shape[a] for a in ("seq", "section", "tp"))
    program = functools.partial(chained, *counts) if counts[0] == 2 else body
    placed = (
        P("seq"),
        P(("tp", "seq"), None),
        P("section", None),
        P("section", "seq", "tp"),
        P("section", "seq", "tp"),
    )
    return jax.shard_map(
        program, mesh=mesh, in_specs=placed, out_specs=P("section", "seq", "tp"), check_vma=False
    )
```

```python
import functools

import jax
import jax.numpy as jnp
from jax import lax
from jax.experimental import pallas as pl
from jax.experimental.pallas import tpu as pltpu
from jax.sharding import PartitionSpec as P

QUERY_HEADS = 16
KEY_VALUE_HEADS = 8
HEAD_WIDTH = 128


EPS = 1e-05
ROPE_BASE = 500000.0
MASKED = -1e30


def passed_along(value, axis, steps):
    count = lax.axis_size(axis)
    leading, last = (max(0, -steps), min(count, count - steps))
    return lax.ppermute(value, axis, [(source, source + steps) for source in range(leading, last)])


def from_root(value, axis, root):
    mine = lax.axis_index(axis) == root
    return lax.psum(jnp.where(mine, value, jnp.zeros_like(value)), axis)


def rope_tables(positions, head_size):
    half_width = head_size // 2
    inverse_freq = ROPE_BASE ** (-jnp.arange(half_width).astype(jnp.float32) * (2.0 / head_size))
    angles = positions.astype(jnp.float32)[:, None] * inverse_freq[None, :]
    return (jnp.cos(angles), jnp.sin(angles))


def rotate_half(heads, cosine_table, sine_values):
    half_width = heads.shape[-1] // 2
    first_half = heads[..., :half_width]
    second = heads[..., half_width:]
    cosine_table = cosine_table[:, None, :]
    sine_values = sine_values[:, None, :]
    return jnp.concatenate(
        [
            first_half * cosine_table - second * sine_values,
            second * cosine_table + first_half * sine_values,
        ],
        axis=-1,
    )


def norm_rows(row_block, gain_row):
    values = row_block.astype(jnp.float32)
    inverse_rms = lax.rsqrt(jnp.mean(values * values, axis=-1, keepdims=True) + EPS)
    return (values * inverse_rms * gain_row[None, :]).astype(jnp.bfloat16)


def widen(current):
    return lax.all_gather(current, "tp", axis=1, tiled=True)


def project(full_rows, gain_row, qkv_full, positions, query_heads, key_value_heads):
    row_count = full_rows.shape[0]
    normed = norm_rows(full_rows, gain_row)
    projected_rows = jnp.dot(normed, qkv_full, preferred_element_type=jnp.float32)
    projected_rows = projected_rows.reshape(
        row_count, query_heads + 2 * key_value_heads, HEAD_WIDTH
    )
    cosine_table, sine_values = rope_tables(positions, HEAD_WIDTH)
    query_rows = rotate_half(projected_rows[:, :query_heads], cosine_table, sine_values).astype(
        jnp.bfloat16
    )
    key_head_rows = rotate_half(
        projected_rows[:, query_heads : query_heads + key_value_heads], cosine_table, sine_values
    ).astype(jnp.bfloat16)
    value_head_rows = projected_rows[:, query_heads + key_value_heads :].astype(jnp.bfloat16)
    return (query_rows, key_head_rows, value_head_rows)


def attend(query_rows, key_head_rows, value_head_rows, allowed):
    row_count, query_heads, head_size = query_rows.shape
    key_value_heads = key_head_rows.shape[1]
    query_groups = query_rows.reshape(
        row_count, key_value_heads, query_heads // key_value_heads, head_size
    )
    scores = jnp.einsum(
        "rkph,ckh->kprc", query_groups, key_head_rows, preferred_element_type=jnp.float32
    ) * head_size ** (-0.5)
    scores = jnp.where(allowed[None, None], scores, MASKED)
    weights = jax.nn.softmax(scores, axis=-1).astype(jnp.bfloat16)
    attended = jnp.einsum(
        "kprc,ckh->rkph", weights, value_head_rows, preferred_element_type=jnp.float32
    )
    return attended.reshape(row_count, query_heads * head_size).astype(jnp.bfloat16)


def combine(current, attended, out_full):
    partial_value = lax.dot_general(
        attended, out_full, (((1,), (1,)), ((), ())), preferred_element_type=jnp.float32
    )
    summed = lax.psum_scatter(
        partial_value.astype(jnp.bfloat16), "tp", scatter_dimension=1, tiled=True
    ).astype(jnp.float32)
    return (current.astype(jnp.float32) + summed).astype(jnp.bfloat16)


def advance(new_rows):
    return passed_along(new_rows, "section", 1)


def body(token_ids, embed_columns, norm_gain, qkv_weight, out_weight):
    seq_count = lax.axis_size("seq")
    section_count = lax.axis_size("section")
    tensor_parallel_count = lax.axis_size("tp")
    group_index = lax.axis_index("seq")
    section_index = lax.axis_index("section")
    block_row_slice = token_ids.shape[0]
    feature_slice = embed_columns.shape[0]
    feature_cols = feature_slice * seq_count
    query_heads = QUERY_HEADS // tensor_parallel_count
    key_value_heads = KEY_VALUE_HEADS // tensor_parallel_count
    every_id = lax.all_gather(token_ids, "seq", axis=0, tiled=True)
    looked = jnp.take(embed_columns, every_id, axis=1)
    arrived = lax.all_to_all(looked, "seq", split_axis=1, concat_axis=0, tiled=True)
    residual = arrived.T
    qkv_full, out_full = (
        lax.all_gather(qkv_weight, "seq", axis=1, tiled=True),
        lax.all_gather(out_weight, "seq", axis=1, tiled=True),
    )
    qkv_full = qkv_full[0]
    out_full = out_full[0]
    gain_row = norm_gain[0].astype(jnp.float32)
    outputs = jnp.zeros((block_row_slice, feature_cols), jnp.bfloat16)
    row_ids = jnp.arange(block_row_slice)[:, None]
    column = jnp.arange(2 * block_row_slice)[None, :]
    positions = group_index * block_row_slice + jnp.arange(block_row_slice)
    allowed = jnp.where(
        column < block_row_slice, group_index > 0, column - block_row_slice <= row_ids
    )
    current = residual
    for step_number in range(section_count):
        query_rows, key_head_rows, value_head_rows = project(
            widen(current), gain_row, qkv_full, positions, query_heads, key_value_heads
        )
        anchor_heads, anchor_values = (
            from_root(key_head_rows, "seq", 0),
            from_root(value_head_rows, "seq", 0),
        )
        both_keys = jnp.concatenate([anchor_heads, key_head_rows], axis=0)
        both_values = jnp.concatenate([anchor_values, value_head_rows], axis=0)
        attended = attend(query_rows, both_keys, both_values, allowed)
        new_rows = combine(current, attended, out_full)
        outputs = jnp.where(section_index == step_number, new_rows, outputs)
        if step_number + 1 < section_count:
            current = advance(new_rows)
    return outputs[None]


LANES = 128
TOKEN_GROUP = 8
MESH = pl.DeviceIdType.MESH


def lookup_kernel(mine_ref, theirs_ref, table_ref, out_ref, tiles, sems):
    count = out_ref.shape[0]
    width = table_ref.shape[0]
    block = mine_ref.shape[0]
    first = lax.axis_index("section") * count
    ours = first // block == lax.axis_index("seq")
    ids = [
        jnp.where(ours, mine_ref[first % block + i], theirs_ref[first % block + i])
        for i in range(count)
    ]

    def fetch(i):
        start = pl.multiple_of((ids[i] // LANES) * LANES, LANES)
        return pltpu.make_async_copy(
            table_ref.at[:, pl.ds(start, LANES)], tiles.at[:, pl.ds(i * LANES, LANES)], sems.at[i]
        )

    for i in range(count):
        fetch(i).start()
    rows = lax.broadcasted_iota(jnp.int32, (LANES, LANES), 0)
    columns = lax.broadcasted_iota(jnp.int32, (LANES, LANES), 1)
    total = jnp.zeros((width, LANES), jnp.float32)
    group = min(TOKEN_GROUP, count)
    for base in range(0, count, group):
        picks = []
        for i in range(base, base + group):
            chosen = jnp.logical_and(rows == ids[i] % LANES, columns == i)
            picks.append(jnp.where(chosen, 1.0, 0.0).astype(jnp.bfloat16))
        pick = jnp.concatenate(picks, axis=0)
        for i in range(base, base + group):
            fetch(i).wait()
        total += jnp.dot(
            tiles[:, base * LANES : (base + group) * LANES], pick, preferred_element_type=jnp.float32
        )
    out_ref[...] = total.T[:count].astype(jnp.bfloat16)


def chain_kernel(
    n_seq,
    n_sec,
    n_tp,
    piece_ref,
    gain_ref,
    cos_ref,
    sin_ref,
    qkv_ref,
    outw_ref,
    out_ref,
    wq,
    wo,
    hidden,
    acc,
    part_send,
    part_recv,
    sq_send,
    sq_recv,
    kept,
    heads,
    rs_send,
    rs_recv,
    fresh,
    w_sem,
    h_ssem,
    h_rsem,
    p_ssem,
    p_rsem,
    q_ssem,
    q_rsem,
    r_ssem,
    r_rsem,
    o_ssem,
    o_rsem,
):
    seq, sec, tp = (lax.axis_index(a) for a in ("seq", "section", "tp"))
    tokens, chunk = fresh.shape
    piece = tokens // n_sec
    block = out_ref.shape[1]
    _, groups, _, group_width = part_send.shape
    query_heads = QUERY_HEADS // n_tp
    kv_heads = KEY_VALUE_HEADS // n_tp

    load_q = [
        pltpu.make_async_copy(
            qkv_ref.at[0, pl.ds(((tp + d) % n_tp) * chunk, chunk), :],
            wq.at[pl.ds(((tp + d) % n_tp) * chunk, chunk), :],
            w_sem.at[d],
        )
        for d in range(n_tp)
    ]
    load_o = pltpu.make_async_copy(outw_ref.at[0], wo, w_sem.at[n_tp])
    for c in load_q:
        c.start()
    load_o.start()

    shard = tp * n_seq + seq
    half, slot = shard // n_tp, shard % n_tp

    def seed_copy(j):
        return pltpu.make_async_remote_copy(
            src_ref=piece_ref,
            dst_ref=hidden.at[slot, pl.ds(sec * piece, piece), :],
            send_sem=h_ssem.at[0, j],
            recv_sem=h_rsem.at[slot, sec],
            device_id={"seq": half, "section": 0, "tp": j},
            device_id_type=MESH,
        )

    def seed_is_mine(j):
        return jnp.logical_and(sec == 0, jnp.logical_and(half == seq, tp == j))

    seed_local = pltpu.make_async_copy(
        piece_ref, hidden.at[slot, pl.ds(sec * piece, piece), :], h_rsem.at[slot, sec]
    )
    for j in range(n_tp):
        mine = seed_is_mine(j)

        @pl.when(mine)
        def _():
            seed_local.start()

        @pl.when(jnp.logical_not(mine))
        def _():
            seed_copy(j).start()

    other = 1 - seq
    pieces = block // piece

    def square_copy(p):
        return pltpu.make_async_remote_copy(
            src_ref=sq_send.at[p],
            dst_ref=sq_recv.at[p],
            send_sem=q_ssem.at[p],
            recv_sem=q_rsem.at[p],
            device_id={"seq": other},
            device_id_type=MESH,
        )

    def part_copy(p, g):
        return pltpu.make_async_remote_copy(
            src_ref=part_send.at[p, g],
            dst_ref=part_recv.at[p, g],
            send_sem=p_ssem.at[p, g],
            recv_sem=p_rsem.at[p, g],
            device_id={"seq": other},
            device_id_type=MESH,
        )

    def rs_copy(p, d):
        return pltpu.make_async_remote_copy(
            src_ref=rs_send.at[p, d],
            dst_ref=rs_recv.at[p, d],
            send_sem=r_ssem.at[p, d],
            recv_sem=r_rsem.at[p, d],
            device_id={"tp": (tp + d) % n_tp},
            device_id_type=MESH,
        )

    def next_copy(d, k):
        return pltpu.make_async_remote_copy(
            src_ref=fresh.at[pl.ds(k * piece, piece), :],
            dst_ref=hidden.at[tp, pl.ds(k * piece, piece), :],
            send_sem=h_ssem.at[k + 1, d],
            recv_sem=h_rsem.at[tp, k],
            device_id={"section": sec + 1, "tp": (tp + n_tp - d) % n_tp},
            device_id_type=MESH,
        )

    place = seq * n_tp + tp
    holder, part_of = place // n_seq, place % n_seq

    def out_copy(b):
        return pltpu.make_async_remote_copy(
            src_ref=fresh.at[pl.ds(b * block, block), :],
            dst_ref=out_ref.at[0, :, pl.ds(pl.multiple_of(part_of * chunk, chunk), chunk)],
            send_sem=o_ssem.at[b],
            recv_sem=o_rsem.at[part_of],
            device_id={"seq": b, "tp": holder},
            device_id_type=MESH,
        )

    def project(p):
        span = slice(p * block, (p + 1) * block)
        squares = jnp.zeros((block, LANES), jnp.float32)
        for d in range(n_tp):
            c = (tp + d) % n_tp
            for k in range(p * pieces, (p + 1) * pieces):
                view = hidden.at[c, pl.ds(k * piece, piece), :]
                pltpu.make_async_copy(view, view, h_rsem.at[c, k]).wait()
            if p == 0:
                load_q[d].wait()
            rows = hidden[c, span, :].astype(jnp.float32)
            sq = rows * rows
            for k in range(chunk // LANES):
                squares += sq[:, k * LANES : (k + 1) * LANES]
            at = pl.multiple_of(seq * (n_tp * chunk) + c * chunk, chunk)
            gain = gain_ref[:, pl.ds(at, chunk)].astype(jnp.float32)
            scaled = (rows * gain).astype(jnp.bfloat16)
            if d == n_tp - 1:
                sq_send[p] = squares
                square_copy(p).start()
            for g in range(groups):
                cols = slice(g * group_width, (g + 1) * group_width)
                product = jnp.dot(
                    scaled,
                    wq[pl.ds(pl.multiple_of(c * chunk, chunk), chunk), cols],
                    preferred_element_type=jnp.float32,
                )
                if d > 0:
                    product += acc[span, cols]
                acc[span, cols] = product
                if d == n_tp - 1:
                    part_send[p, g] = product.astype(jnp.bfloat16)
                    part_copy(p, g).start()

    repeat = query_heads // kv_heads

    def attend_block(p):
        span = slice(p * block, (p + 1) * block)
        square_copy(p).wait_recv()
        features = n_seq * n_tp * chunk
        mean = jnp.sum(sq_send[p] + sq_recv[p], axis=-1, keepdims=True) * (1.0 / features)
        inverse_rms = lax.rsqrt(mean + EPS)
        cosine, sine = cos_ref[span, :], sin_ref[span, :]
        ready = []
        for g in range(groups):
            part_copy(p, g).wait_recv()
            cols = slice(g * group_width, (g + 1) * group_width)
            whole = (acc[span, cols] + part_recv[p, g].astype(jnp.float32)) * inverse_rms
            for k in range(group_width // HEAD_WIDTH):
                head = whole[:, k * HEAD_WIDTH : (k + 1) * HEAD_WIDTH]
                if len(ready) < query_heads + kv_heads:
                    head = head * cosine + pltpu.roll(head, HEAD_WIDTH // 2, 1) * sine
                head = head.astype(jnp.bfloat16)
                if len(ready) >= query_heads:
                    kept[len(ready) - query_heads, span, :] = head
                ready.append(head)
        known = (p + 1) * block
        row_at = lax.broadcasted_iota(jnp.int32, (repeat, block, known), 1)
        key_at = lax.broadcasted_iota(jnp.int32, (repeat, block, known), 2)
        visible = (key_at <= row_at + p * block).reshape(repeat * block, known)
        for h in range(kv_heads):
            queries = jnp.concatenate(ready[h * repeat : (h + 1) * repeat], axis=0)
            scores = lax.dot_general(
                queries, kept[h, :known, :], (((1,), (1,)), ((), ())), preferred_element_type=jnp.float32
            ) * HEAD_WIDTH ** (-0.5)
            scores = jnp.where(visible, scores, MASKED)
            shifted = jnp.exp(scores - jnp.max(scores, axis=-1, keepdims=True))
            weights = (shifted / jnp.sum(shifted, axis=-1, keepdims=True)).astype(jnp.bfloat16)
            attended = jnp.dot(
                weights, kept[kv_heads + h, :known, :], preferred_element_type=jnp.float32
            ).astype(jnp.bfloat16)
            for r in range(repeat):
                at = (h * repeat + r) * HEAD_WIDTH
                heads[span, at : at + HEAD_WIDTH] = attended[r * block : (r + 1) * block]
        if p == 0:
            load_o.wait()
        attended = heads[span, :]
        for d in [*range(1, n_tp), 0]:
            c = (tp + d) % n_tp
            partial = lax.dot_general(
                attended,
                wo[pl.ds(pl.multiple_of(c * chunk, chunk), chunk), :],
                (((1,), (1,)), ((), ())),
                preferred_element_type=jnp.float32,
            ).astype(jnp.bfloat16)
            rs_send[p, d] = partial
            if d:
                rs_copy(p, d).start()

    def forward(p):
        span = slice(p * block, (p + 1) * block)
        summed = rs_send[p, 0].astype(jnp.float32)
        for d in range(1, n_tp):
            rs_copy(p, d).wait_recv()
            summed += rs_recv[p, d].astype(jnp.float32)
        fresh[span, :] = (hidden[tp, span, :].astype(jnp.float32) + summed).astype(jnp.bfloat16)

        @pl.when(sec < n_sec - 1)
        def _():
            for d in range(n_tp):
                for k in range(p * pieces, (p + 1) * pieces):
                    next_copy(d, k).start()

        mine = jnp.logical_and(seq == p, holder == tp)

        @pl.when(mine)
        def _():
            pltpu.make_async_copy(
                fresh.at[pl.ds(seq * block, block), :],
                out_ref.at[0, :, pl.ds(pl.multiple_of(part_of * chunk, chunk), chunk)],
                o_rsem.at[part_of],
            ).start()

        @pl.when(jnp.logical_not(mine))
        def _():
            out_copy(p).start()

    project(0)
    attend_block(0)
    forward(0)
    project(1)
    attend_block(1)
    forward(1)

    for p in range(n_seq):
        view = out_ref.at[0, :, pl.ds(p * chunk, chunk)]
        pltpu.make_async_copy(view, view, o_rsem.at[p]).wait()

    for p in range(n_seq):

        @pl.when(jnp.logical_not(jnp.logical_and(seq == p, holder == tp)))
        def _():
            out_copy(p).wait_send()

    @pl.when(sec < n_sec - 1)
    def _():
        for d in range(n_tp):
            for k in range(n_sec):
                next_copy(d, k).wait_send()

    for p in range(n_seq):
        for d in range(1, n_tp):
            rs_copy(p, d).wait_send()
        for g in range(groups):
            part_copy(p, g).wait_send()
        square_copy(p).wait_send()
    for j in range(n_tp):

        @pl.when(jnp.logical_not(seed_is_mine(j)))
        def _():
            seed_copy(j).wait_send()


def chained(n_seq, n_sec, n_tp, token_ids, embed_columns, norm_gain, qkv_weight, out_weight):
    block = token_ids.shape[0]
    tokens = block * n_seq
    chunk = embed_columns.shape[0]
    columns = qkv_weight.shape[2]
    half = qkv_weight.shape[1]
    piece = tokens // n_sec
    groups = 4
    theirs = lax.ppermute(token_ids, "seq", [(0, 1), (1, 0)])
    looked = pl.pallas_call(
        lookup_kernel,
        out_shape=jax.ShapeDtypeStruct((piece, chunk), jnp.bfloat16),
        in_specs=[
            pl.BlockSpec(memory_space=pltpu.SMEM),
            pl.BlockSpec(memory_space=pltpu.SMEM),
            pl.BlockSpec(memory_space=pltpu.HBM),
        ],
        out_specs=pl.BlockSpec(memory_space=pltpu.VMEM),
        scratch_shapes=[
            pltpu.VMEM((chunk, piece * LANES), jnp.bfloat16),
            pltpu.SemaphoreType.DMA((piece,)),
        ],
    )(token_ids, theirs, embed_columns)
    cosine, sine = rope_tables(jnp.arange(tokens), HEAD_WIDTH)
    cosine = jnp.concatenate([cosine, cosine], axis=1)
    sine = jnp.concatenate([-sine, sine], axis=1)
    vmem = pl.BlockSpec(memory_space=pltpu.VMEM)
    hbm = pl.BlockSpec(memory_space=pltpu.HBM)
    dma = pltpu.SemaphoreType.DMA
    return pl.pallas_call(
        functools.partial(chain_kernel, n_seq, n_sec, n_tp),
        out_shape=jax.ShapeDtypeStruct((1, block, n_seq * chunk), jnp.bfloat16),
        in_specs=[vmem, vmem, vmem, vmem, hbm, hbm],
        out_specs=vmem,
        scratch_shapes=[
            pltpu.VMEM((half, columns), jnp.bfloat16),
            pltpu.VMEM((half, out_weight.shape[2]), jnp.bfloat16),
            pltpu.VMEM((n_tp, tokens, chunk), jnp.bfloat16),
            pltpu.VMEM((tokens, columns), jnp.float32),
            pltpu.VMEM((n_seq, groups, block, columns // groups), jnp.bfloat16),
            pltpu.VMEM((n_seq, groups, block, columns // groups), jnp.bfloat16),
            pltpu.VMEM((n_seq, block, LANES), jnp.float32),
            pltpu.VMEM((n_seq, block, LANES), jnp.float32),
            pltpu.VMEM((2 * KEY_VALUE_HEADS // n_tp, tokens, HEAD_WIDTH), jnp.bfloat16),
            pltpu.VMEM((tokens, out_weight.shape[2]), jnp.bfloat16),
            pltpu.VMEM((n_seq, n_tp, block, chunk), jnp.bfloat16),
            pltpu.VMEM((n_seq, n_tp, block, chunk), jnp.bfloat16),
            pltpu.VMEM((tokens, chunk), jnp.bfloat16),
            dma((n_tp + 1,)),
            dma((n_sec + 1, n_tp)),
            dma((n_tp, n_sec)),
            dma((n_seq, groups)),
            dma((n_seq, groups)),
            dma((n_seq,)),
            dma((n_seq,)),
            dma((n_seq, n_tp)),
            dma((n_seq, n_tp)),
            dma((n_seq,)),
            dma((n_seq,)),
        ],
        compiler_params=pltpu.CompilerParams(has_side_effects=True),
    )(looked, norm_gain, cosine, sine, qkv_weight, out_weight)


def solution(mesh):
    counts = tuple(mesh.shape[a] for a in ("seq", "section", "tp"))
    program = functools.partial(chained, *counts) if counts[0] == 2 else body
    placed = (
        P("seq"),
        P(("tp", "seq"), None),
        P("section", None),
        P("section", "seq", "tp"),
        P("section", "seq", "tp"),
    )
    return jax.shard_map(
        program, mesh=mesh, in_specs=placed, out_specs=P("section", "seq", "tp"), check_vma=False
    )
```
